32 devices in a mesh: seq: 8 (over y, x, core), batch: 4 (over z).
Axes of the slice: x: 2, y: 2, z: 4, core: 2. Of those that a mesh axis runs over, the one named last changes fastest.
Arguments:
- query_rows: bfloat16 [4, 1024, 2048], P('batch', 'seq'), may hold values from -6 to 6, as said below
- key_rows: bfloat16 [4, 1024, 1024], P('batch', 'seq'), may hold values from -6 to 6, as said below
- value_rows: bfloat16 [4, 1024, 1024], P('batch', 'seq'), may hold values from -6 to 6, as said below
- attn_output: bfloat16 [4, 1024, 2048], P('batch', 'seq'), may hold values from -6 to 6, as said below
- output_grad: bfloat16 [4, 1024, 2048], P('batch', 'seq'), may hold values from -6 to 6
- log_norm: float32 [4, 16, 1024], P('batch', None, 'seq'), as said below
- slab_order: int32 [4, 8], P('batch', 'seq'), may hold values from 0 to 7, as said below
- normed_input: bfloat16 [4, 1024, 4608], P('batch', 'seq'), may hold values from -6 to 6
Outputs:
- grad_query: bfloat16 [4, 1024, 2048], P('batch', 'seq')
- grad_key: bfloat16 [4, 1024, 1024], P('batch', 'seq')
- grad_weight: float32 [4608, 1024], P('seq')
The draws below stay inside these ranges and needn't reach their ends.
Inputs may be any that keep to these rules, and one draw needn't show every extreme that they name: `query_rows`: queries of a causal forward pass with 16 heads. `key_rows`: keys of the same forward pass with 8 heads. `value_rows`: values of the same forward pass. `attn_output`: the forward pass's output: for each head, sum over keys at or before the query's position of exp(score - log_norm) times the value. `log_norm`: log of the sum of exp(score) over the keys at or before the query's position, so that each row's weights sum to one. `slab_order`: each row is a permutation of the slab places.
All inputs are finite; a program needn't handle non-finite values.
Results may differ from the reference program's by a relative error of at most 0.025.
Values may be sent and summed in bfloat16 or wider, within the bound.
A program may use at most 128 MiB of HBM per device.

```python
import jax
import jax.numpy as jnp
from jax import lax

D = 4608
HEADS = 16
KV_HEADS = 8
HEAD = 128
TOK_DEV = 128
LENGTH = 1024
BATCH = 4


SCALE = 144.0 ** (-0.5)


def slab_places(key):
    base = jax.random.fold_in(key, 11)
    subkeys = jax.random.split(base, BATCH)
    return jax.vmap(lambda subkey: jax.random.permutation(subkey, LENGTH // TOK_DEV))(subkeys).astype(jnp.int32)


def one_draw(subkey, width):
    values = jax.random.normal(subkey, (BATCH, LENGTH, width), jnp.float32)
    return jnp.clip(values, -6.0, 6.0).astype(jnp.bfloat16)


def projections(key):
    base = jax.random.fold_in(key, 23)
    first, second, third = jax.random.split(base, 3)
    return (one_draw(first, HEADS * HEAD), one_draw(second, KV_HEADS * HEAD), one_draw(third, KV_HEADS * HEAD))


def forward(key):
    queries, keys, values = projections(key)
    order = slab_places(key)
    group = HEADS // KV_HEADS

    def sequence(inputs):
        query_seq, key_seq, value_seq, order_row = inputs
        positions = (order_row[:, None] * TOK_DEV + jnp.arange(TOK_DEV, dtype=jnp.int32)[None, :]).reshape(LENGTH)
        query_f = query_seq.astype(jnp.float32).reshape(LENGTH, KV_HEADS, group, HEAD)
        key_f = key_seq.astype(jnp.float32).reshape(LENGTH, KV_HEADS, HEAD)
        value_f = value_seq.astype(jnp.float32).reshape(LENGTH, KV_HEADS, HEAD)
        scores = SCALE * jnp.einsum('tgrd,kgd->grtk', query_f, key_f)
        allowed = positions[None, :] <= positions[:, None]
        scores = jnp.where(allowed, scores, -1e+30)
        top = jnp.max(scores, axis=3, keepdims=True)
        weights = jnp.where(allowed, jnp.exp(scores - top), 0.0)
        total = jnp.sum(weights, axis=3, keepdims=True)
        outputs = jnp.einsum('grtk,kgd->tgrd', weights / total, value_f)
        norms = (top + jnp.log(total))[..., 0].reshape(HEADS, LENGTH)
        return (outputs.reshape(LENGTH, HEADS * HEAD).astype(jnp.bfloat16), norms)
    return lax.map(sequence, (queries, keys, values, order))


def draw_query_rows(key, part):
    return projections(key)[0]


def draw_key_rows(key, part):
    return projections(key)[1]


def draw_value_rows(key, part):
    return projections(key)[2]


def draw_attn_output(key, part):
    return forward(key)[0]


def draw_log_norm(key, part):
    return forward(key)[1]


def draw_slab_order(key, part):
    return slab_places(key)


def level_of(own_key, shape, shards, smallest, top_value):
    level = 1.0
    for dim, blocks in shards:
        heights = jax.random.uniform(jax.random.fold_in(jax.random.fold_in(own_key, 6), dim), (blocks,), jnp.float32, smallest / len(shards), top_value / len(shards))
        level = level * jnp.repeat(jnp.exp(heights), shape[dim] // blocks).reshape((-1,) + (1,) * (len(shape) - 1 - dim))
    return level


def scatter_about(stream_key, extent, scale, limit, shards=(), kind=jnp.bfloat16):
    drawn = jax.random.normal(stream_key, extent, jnp.float32) * scale
    if len(shards) > 0:
        drawn = level_of(stream_key, extent, shards, -0.22, 0.18) * drawn
    return jnp.clip(drawn, min=-limit, max=limit).astype(kind)


def setup_inputs(seed: int = 0) -> dict:
    seeds = jax.random.split(jax.random.key(seed), 9)
    return {
        "query_rows": draw_query_rows(jax.random.fold_in(seeds[8], 71), 0),
        "key_rows": draw_key_rows(jax.random.fold_in(seeds[8], 71), 0),
        "value_rows": draw_value_rows(jax.random.fold_in(seeds[8], 71), 0),
        "attn_output": draw_attn_output(jax.random.fold_in(seeds[8], 71), 0),
        "output_grad": scatter_about(seeds[4], (BATCH, LENGTH, HEADS * HEAD), 1.0, 6.0, ((0, 4), (1, 8))),
        "log_norm": draw_log_norm(jax.random.fold_in(seeds[8], 71), 0),
        "slab_order": draw_slab_order(jax.random.fold_in(seeds[8], 71), 0),
        "normed_input": scatter_about(seeds[7], (BATCH, LENGTH, D), 1.0, 6.0, ((0, 4), (1, 8))),
    }


SCALE = 144.0 ** -0.5


def rounded(values):
    return lax.optimization_barrier(values.astype(jnp.bfloat16)).astype(jnp.float32)


def block_terms(query_rows, output_rows, grad_rows, norm_rows, query_pos, key_rows, value_rows, key_pos):
    count = query_rows.shape[0]
    keys_count = key_rows.shape[0]
    group = HEADS // KV_HEADS
    queries = query_rows.astype(jnp.float32).reshape(count, KV_HEADS, group, HEAD)
    grads = grad_rows.astype(jnp.float32).reshape(count, KV_HEADS, group, HEAD)
    outputs = output_rows.astype(jnp.float32).reshape(count, KV_HEADS, group, HEAD)
    keys = key_rows.astype(jnp.float32).reshape(keys_count, KV_HEADS, HEAD)
    values = value_rows.astype(jnp.float32).reshape(keys_count, KV_HEADS, HEAD)
    norms = norm_rows.reshape(KV_HEADS, group, count)
    delta = jnp.transpose(jnp.sum(grads * outputs, axis=3), (1, 2, 0))
    scores = SCALE * jnp.einsum('tgrd,kgd->grtk', queries, keys)
    allowed = key_pos[None, :] <= query_pos[:, None]
    probs = jnp.where(allowed, jnp.exp(scores - norms[..., None]), 0.0)
    dprob = jnp.einsum('tgrd,kgd->grtk', grads, values)
    dscore = probs * (dprob - delta[..., None])
    probs_low = rounded(probs)
    dscore_low = rounded(dscore)
    grad_q = SCALE * jnp.einsum('grtk,kgd->tgrd', dscore_low, keys)
    grad_k = SCALE * jnp.einsum('grtk,tgrd->kgd', dscore_low, queries)
    grad_v = jnp.einsum('grtk,tgrd->kgd', probs_low, grads)
    return (grad_q.reshape(count, HEADS * HEAD),
            grad_k.reshape(keys_count, KV_HEADS * HEAD),
            grad_v.reshape(keys_count, KV_HEADS * HEAD))


def reference(query_rows, key_rows, value_rows, attn_output, output_grad, log_norm, slab_order, normed_input):
    slabs = LENGTH // TOK_DEV
    kv_width = KV_HEADS * HEAD

    def sequence(weight, inputs):
        queries, keys, values, outputs, grads, norms, order, normed = inputs
        positions = (order[:, None].astype(jnp.int32) * TOK_DEV
                     + jnp.arange(TOK_DEV, dtype=jnp.int32)[None, :]).reshape(LENGTH)

        def per_slab(carry, index):
            acc_key, acc_value = carry
            start = (index * TOK_DEV).astype(jnp.int32)
            grad_q, grad_k, grad_v = block_terms(
                lax.dynamic_slice_in_dim(queries, start, TOK_DEV, 0),
                lax.dynamic_slice_in_dim(outputs, start, TOK_DEV, 0),
                lax.dynamic_slice_in_dim(grads, start, TOK_DEV, 0),
                lax.dynamic_slice_in_dim(norms, start, TOK_DEV, 1),
                lax.dynamic_slice_in_dim(positions, start, TOK_DEV, 0),
                keys, values, positions)
            return (acc_key + rounded(grad_k), acc_value + rounded(grad_v)), grad_q.astype(jnp.bfloat16)

        zeros = jnp.zeros((LENGTH, kv_width), jnp.float32)
        (acc_key, acc_value), slab_query = lax.scan(per_slab, (zeros, zeros), jnp.arange(slabs, dtype=jnp.int32))
        grad_query = slab_query.reshape(LENGTH, HEADS * HEAD)
        grad_key = acc_key.astype(jnp.bfloat16)
        grad_value = acc_value.astype(jnp.bfloat16).astype(jnp.float32)

        def per_weight(total, index):
            start = (index * TOK_DEV).astype(jnp.int32)
            rows_in = lax.dynamic_slice_in_dim(normed, start, TOK_DEV, 0).astype(jnp.float32)
            rows_grad = lax.dynamic_slice_in_dim(grad_value, start, TOK_DEV, 0)
            part = jnp.dot(rows_in.T, rows_grad, preferred_element_type=jnp.float32)
            return total + rounded(part), None

        weight, _ = lax.scan(per_weight, weight, jnp.arange(slabs, dtype=jnp.int32))
        return weight, (grad_query, grad_key)

    start_weight = jnp.zeros((D, kv_width), jnp.float32)
    weight, (grad_query, grad_key) = lax.scan(
        sequence, start_weight,
        (query_rows, key_rows, value_rows, attn_output, output_grad, log_norm, slab_order, normed_input))
    return grad_query, grad_key, weight
```

```python
import functools
import math

import jax
import jax.numpy as jnp
from jax import lax
from jax.experimental import pallas as pl
from jax.experimental.pallas import tpu as pltpu
from jax.sharding import PartitionSpec as P

HEADS = 16
KV_HEADS = 8
HEAD = 128


SCALE = 144.0 ** (-0.5)


def block_terms(queries, grads, delta, norms, query_pos, key_block, value_block, key_pos):
    keys_count = key_block.shape[0]
    scores = SCALE * jnp.einsum(
        "tgrd,kgd->grtk", queries, key_block, preferred_element_type=jnp.float32
    )
    allowed = key_pos[None, :] <= query_pos[:, None]
    probs = jnp.where(allowed, jnp.exp(scores - norms[..., None]), 0.0)
    dprob = jnp.einsum("tgrd,kgd->grtk", grads, value_block, preferred_element_type=jnp.float32)
    dscore = probs * (dprob - delta[..., None])
    probs_low = probs.astype(jnp.bfloat16)
    dscore_low = dscore.astype(jnp.bfloat16)
    grad_q = SCALE * jnp.einsum(
        "grtk,kgd->tgrd", dscore_low, key_block, preferred_element_type=jnp.float32
    )
    grad_k = SCALE * jnp.einsum(
        "grtk,tgrd->kgd", dscore_low, queries, preferred_element_type=jnp.float32
    )
    grad_v = jnp.einsum("grtk,tgrd->kgd", probs_low, grads, preferred_element_type=jnp.float32)
    return (grad_q, grad_k.reshape(keys_count, -1), grad_v.reshape(keys_count, -1))


def local(
    query_rows, key_rows, value_rows, attn_output, output_grad, log_norm, slab_order, normed_input
):
    tokens = query_rows.shape[1]
    group = HEADS // KV_HEADS
    kv_width = KV_HEADS * HEAD
    slabs = lax.axis_size("seq")
    length = tokens * slabs
    orders = lax.all_gather(slab_order, "seq", axis=1, tiled=True)
    queries = query_rows[0].reshape(tokens, KV_HEADS, group, HEAD)
    grads = output_grad[0].reshape(tokens, KV_HEADS, group, HEAD)
    outputs = attn_output[0].reshape(tokens, KV_HEADS, group, HEAD)
    delta = jnp.transpose(
        jnp.sum(grads.astype(jnp.float32) * outputs.astype(jnp.float32), axis=3), (1, 2, 0)
    )
    norms = log_norm[0].reshape(KV_HEADS, group, tokens)
    offsets = jnp.arange(tokens, dtype=jnp.int32)
    query_pos = slab_order[0, 0] * tokens + offsets
    width = tokens * -(-512 // tokens)
    empty_kv = jnp.zeros((length, kv_width), jnp.float32)
    empty_q = jnp.zeros((tokens, KV_HEADS, group, HEAD), jnp.float32)
    start = jnp.int32(0)
    grad_q = empty_q
    grad_k = empty_kv
    grad_v = empty_kv
    key_part = lax.all_gather(key_rows, "seq", axis=1, tiled=True)
    value_part = lax.all_gather(value_rows, "seq", axis=1, tiled=True)
    count = key_part.shape[1]
    for begin in range(0, count, width):
        finish = min(begin + width, count)
        shards = (finish - begin) // tokens
        first = (start + begin) // tokens
        places = lax.dynamic_slice_in_dim(orders[0], first, shards, 0)
        key_pos = (places[:, None] * tokens + offsets[None, :]).reshape(-1)
        key_block = key_part[0, begin:finish].reshape(-1, KV_HEADS, HEAD)
        value_block = value_part[0, begin:finish].reshape(-1, KV_HEADS, HEAD)
        term_q, term_k, term_v = block_terms(
            queries, grads, delta, norms, query_pos, key_block, value_block, key_pos
        )
        grad_q = grad_q + term_q
        grad_k = lax.dynamic_update_slice_in_dim(grad_k, term_k, begin, 0)
        grad_v = lax.dynamic_update_slice_in_dim(grad_v, term_v, begin, 0)
    grad_q, part_key, part_value = (grad_q, grad_k, grad_v)
    key_sum, value_sum = (
        lax.psum_scatter(
            part_key.astype(jnp.bfloat16), "seq", scatter_dimension=0, tiled=True
        ).astype(jnp.float32),
        lax.psum_scatter(
            part_value.astype(jnp.bfloat16), "seq", scatter_dimension=0, tiled=True
        ).astype(jnp.float32),
    )
    every_grad = lax.all_gather(value_sum.astype(jnp.bfloat16), "seq", axis=0, tiled=True)
    own_columns = lax.all_to_all(normed_input[0], "seq", split_axis=1, concat_axis=0, tiled=True)
    share = own_columns.shape[1]
    slab_parts = jnp.einsum(
        "std,stk->sdk",
        own_columns.reshape(slabs, tokens, share),
        every_grad.reshape(slabs, tokens, kv_width),
        preferred_element_type=jnp.float32,
    )
    rows_total = jnp.sum(slab_parts.astype(jnp.bfloat16).astype(jnp.float32), axis=0)
    weight = lax.psum(rows_total.astype(jnp.bfloat16), "batch").astype(jnp.float32)
    grad_query = grad_q.astype(jnp.bfloat16).reshape(1, tokens, HEADS * HEAD)
    grad_key = key_sum.astype(jnp.bfloat16).reshape(1, tokens, kv_width)
    return (grad_query, grad_key, weight)


MESH = pl.DeviceIdType.MESH
F32 = jnp.float32
BF16 = jnp.bfloat16
NT = (((1,), (1,)), ((), ()))


def xor(a, b, n):
    out = 0
    bit = 1
    while bit < n:
        x, y = lax.rem(lax.div(a, bit), 2), lax.rem(lax.div(b, bit), 2)
        out = out + bit * (x + y - 2 * x * y)
        bit *= 2
    return out


def at(seq, batch):
    return {"seq": seq, "batch": batch}


def window(width, n):
    share = width // n
    step = math.gcd(share, 128)
    return share, -(-(128 - step + share) // 128) * 128


def kernel(
    n, nb, q_ref, k_ref, v_ref, o_ref, g_ref, norm_ref, order_ref, x_ref,
    gq_ref, gk_ref, gw_ref,
    qr, gr, kr, vr, xr, st_src, str_, kt, xt, dk_acc, dv_acc, dq_buf, dk_buf, dv_all,
    prod, up, cr, snd, tot, gq_in, gk_in,
    in_send, in_recv, out_send, out_recv, zu_send, zu_recv, zc_recv, zd_send,
):
    me = lax.axis_index("seq")
    b = lax.axis_index("batch")
    T = k_ref.shape[0]
    H = HEAD
    R = HEADS // KV_HEADS
    share, win = window(x_ref.shape[1], n)
    half = nb // 2
    left = b < half
    is_end = jnp.logical_or(b == 0, b == nb - 1)
    is_mid = jnp.logical_or(b == half - 1, b == half)
    not_end = jnp.logical_not(is_end)
    not_mid = jnp.logical_not(is_mid)
    inner = jnp.where(left, b + 1, b - 1)
    outer = jnp.where(is_end, inner, jnp.where(left, b - 1, b + 1))

    barrier = pltpu.get_barrier_semaphore()
    for t in range(1, n):
        pl.semaphore_signal(barrier, inc=1, device_id=at(xor(me, jnp.int32(t), n), b), device_id_type=MESH)
    pl.semaphore_signal(barrier, inc=1, device_id=at(me, inner), device_id_type=MESH)

    @pl.when(not_end)
    def _():
        pl.semaphore_signal(barrier, inc=1, device_id=at(me, outer), device_id_type=MESH)

    pl.semaphore_wait(barrier, jnp.where(is_end, n, n + 1))

    def cols(who, width):
        return pl.ds(pl.multiple_of(who * width, 128), width)

    def xstart(who):
        return pl.multiple_of(lax.div(who * share, 128) * 128, 128)

    def send_in(kind, t):
        peer = xor(me, jnp.int32(t), n)
        src, dst = {
            0: lambda: (k_ref.at[:, cols(peer, H)], kr.at[me]),
            1: lambda: (v_ref.at[:, cols(peer, H)], vr.at[me]),
            2: lambda: (q_ref.at[:, cols(peer, R * H)], qr.at[me]),
            3: lambda: (g_ref.at[:, cols(peer, R * H)], gr.at[me]),
            4: lambda: (x_ref.at[:, pl.ds(xstart(peer), win)], xr.at[me]),
            5: lambda: (st_src.at[peer], str_.at[me]),
        }[kind]()
        return pltpu.make_async_remote_copy(
            src_ref=src, dst_ref=dst, send_sem=in_send.at[kind, t], recv_sem=in_recv.at[kind, t],
            device_id=at(peer, b), device_id_type=MESH)

    def send_out(kind, t):
        peer = xor(me, jnp.int32(t), n)
        src, dst = {
            0: lambda: (dv_all.at[me], dv_all.at[me]),
            1: lambda: (dk_buf.at[peer], gk_in.at[me]),
            2: lambda: (dq_buf.at[peer], gq_in.at[me]),
        }[kind]()
        return pltpu.make_async_remote_copy(
            src_ref=src, dst_ref=dst, send_sem=out_send.at[kind, t], recv_sem=out_recv.at[kind, t],
            device_id=at(peer, b), device_id_type=MESH)

    for kind in (0, 1):
        for t in range(1, n):
            send_in(kind, t).start()
    for t in range(1, n):
        send_in(2, t).start()
        send_in(3, t).start()

    lane = lax.broadcasted_iota(jnp.int32, (T, 128), 1)
    table = jnp.zeros((T, 128), F32)
    for h in range(HEADS):
        part = g_ref[:, h * H:(h + 1) * H].astype(F32) * o_ref[:, h * H:(h + 1) * H].astype(F32)
        table = jnp.where(lane == h, jnp.sum(part, axis=1, keepdims=True), table)
    delta = jnp.transpose(table)
    base = jnp.full((8 - 2 * R, T), (order_ref[0, 0] * T).astype(F32))
    for h in range(n):
        st_src[h, 0:R, :] = norm_ref[h * R:(h + 1) * R, :]
        st_src[h, R:2 * R, :] = delta[h * R:(h + 1) * R, :]
        st_src[h, 2 * R:8, :] = base
    for t in range(1, n):
        send_in(5, t).start()
    for t in range(1, n):
        send_in(4, t).start()

    kr[me] = k_ref[:, cols(me, H)]
    vr[me] = v_ref[:, cols(me, H)]
    qr[me] = q_ref[:, cols(me, R * H)]
    gr[me] = g_ref[:, cols(me, R * H)]
    xr[me] = x_ref[:, pl.ds(xstart(me), win)]
    str_[me] = st_src[me]
    dk_acc[...] = jnp.zeros_like(dk_acc)
    dv_acc[...] = jnp.zeros_like(dv_acc)

    for t in range(1, n):
        for kind in (0, 1, 5):
            send_in(kind, t).wait_recv()
    for s in range(n):
        kt[:, s * T:(s + 1) * T] = jnp.transpose(kr[s])

    pair = 2 if n % 2 == 0 else 1
    rows = lax.broadcasted_iota(jnp.int32, (T, R * T), 0).astype(F32)
    qoff = lax.broadcasted_iota(jnp.int32, (1, T), 1).astype(F32)

    def wide(i, first):
        return jnp.concatenate([str_[i, first + r:first + r + 1, :] for r in range(R)], axis=1)

    def per_query(t, carry):
        i = xor(me, t, n)

        @pl.when(t > 0)
        def _():
            send_in(2, t).wait_recv()
            send_in(3, t).wait_recv()

        qb, gb = qr[i], gr[i]
        qs = jnp.concatenate([qb[:, r * H:(r + 1) * H] for r in range(R)], axis=0)
        gs = jnp.concatenate([gb[:, r * H:(r + 1) * H] for r in range(R)], axis=0)
        norms, deltas = wide(i, 0), wide(i, R)
        qpos = str_[i, 2 * R:2 * R + 1, :] + qoff
        qpos = jnp.concatenate([qpos] * R, axis=1)
        dqt = jnp.zeros((H, R * T), F32)
        for s in range(0, n, pair):
            kb = kr[s:s + pair].reshape(pair * T, H)
            vb = vr[s:s + pair].reshape(pair * T, H)
            kpos = jnp.concatenate(
                [rows + jnp.concatenate([str_[s + p, 2 * R:2 * R + 1, :]] * R, axis=1) for p in range(pair)],
                axis=0)
            scores = SCALE * lax.dot_general(kb, qs, NT, preferred_element_type=F32)
            probs = jnp.where(kpos <= qpos, jnp.exp(scores - norms), 0.0)
            dprob = lax.dot_general(vb, gs, NT, preferred_element_type=F32)
            low = (probs * (dprob - deltas)).astype(BF16)
            span = slice(s * T, (s + pair) * T)
            dv_acc[span, :] += jnp.dot(probs.astype(BF16), gs, preferred_element_type=F32)
            dk_acc[span, :] += jnp.dot(low, qs, preferred_element_type=F32)
            dqt = dqt + jnp.dot(kt[:, span], low, preferred_element_type=F32)
        dq = jnp.transpose(dqt * SCALE)
        for r in range(R):
            dq_buf[i, :, r * H:(r + 1) * H] = dq[r * T:(r + 1) * T, :].astype(BF16)
        return carry

    lax.fori_loop(0, n, per_query, 0)

    dv_all[me] = dv_acc[...].astype(BF16)
    for t in range(1, n):
        send_out(0, t).start()
    dk_buf[...] = (dk_acc[...] * SCALE).astype(BF16).reshape(dk_buf.shape)
    for kind in (1, 2):
        for t in range(1, n):
            send_out(kind, t).start()

    def turn(t, carry):
        i = xor(me, t, n)

        @pl.when(t > 0)
        def _():
            send_in(4, t).wait_recv()

        xt[:, pl.ds(pl.multiple_of(i * T, 128), T)] = jnp.transpose(xr[i])
        return carry

    lax.fori_loop(0, n, turn, 0)

    off = pl.multiple_of(me * share - xstart(me), math.gcd(share, 128))

    def cross(c):
        return pltpu.make_async_remote_copy(
            src_ref=snd.at[c], dst_ref=cr.at[c], send_sem=zu_send.at[c], recv_sem=zc_recv.at[c],
            device_id=at(me, inner), device_id_type=MESH)

    def inward(c):
        return pltpu.make_async_remote_copy(
            src_ref=snd.at[c], dst_ref=up.at[c], send_sem=zu_send.at[c], recv_sem=zu_recv.at[c],
            device_id=at(me, inner), device_id_type=MESH)

    def outward(c):
        return pltpu.make_async_remote_copy(
            src_ref=tot.at[c], dst_ref=cr.at[c], send_sem=zd_send.at[c], recv_sem=zc_recv.at[c],
            device_id=at(me, outer), device_id_type=MESH)

    def go_up(c):
        @pl.when(c > 0)
        def _():
            send_out(0, c).wait_recv()

        prod[...] = jnp.dot(xt[...], dv_all[xor(me, c, n)], preferred_element_type=F32)

        @pl.when(is_end)
        def _():
            snd[c] = prod[pl.ds(off, share), :].astype(BF16)

        @pl.when(not_end)
        def _():
            inward(c).wait_recv()
            snd[c] = (prod[pl.ds(off, share), :] + up[c].astype(F32)).astype(BF16)

        @pl.when(is_mid)
        def _():
            cross(c).start()

        @pl.when(not_mid)
        def _():
            inward(c).start()

    def go_down(c):
        cross(c).wait_recv()
        head = cols(xor(me, c, n), H)

        @pl.when(is_mid)
        def _():
            tot[c] = (snd[c].astype(F32) + cr[c].astype(F32)).astype(BF16)

        @pl.when(not_mid)
        def _():
            tot[c] = cr[c]

        @pl.when(not_end)
        def _():
            outward(c).start()

        gw_ref[:, head] = tot[c].astype(F32)

    lag = 2

    def z_step(c, carry):
        @pl.when(c < n)
        def _():
            go_up(c)

        @pl.when(c >= lag)
        def _():
            go_down(c - lag)

        return carry

    lax.fori_loop(0, n + lag, z_step, 0)

    gk_ref[:, cols(me, H)] = dk_buf[me]
    gq_ref[:, cols(me, R * H)] = dq_buf[me]

    def collect(t, carry):
        i = xor(me, t, n)
        send_out(1, t).wait_recv()
        send_out(2, t).wait_recv()
        gk_ref[:, cols(i, H)] = gk_in[i]
        gq_ref[:, cols(i, R * H)] = gq_in[i]
        return carry

    lax.fori_loop(1, n, collect, 0)

    def drain(t, carry):
        for kind in range(6):
            send_in(kind, t).wait_send()
        for kind in range(3):
            send_out(kind, t).wait_send()
        return carry

    lax.fori_loop(1, n, drain, 0)

    def drain_z(c, carry):
        cross(c).wait_send()

        @pl.when(not_end)
        def _():
            outward(c).wait_send()

        return carry

    lax.fori_loop(0, n, drain_z, 0)


def by_heads(
    n, nb, query_rows, key_rows, value_rows, attn_output, output_grad, log_norm, slab_order, normed_input
):
    T = query_rows.shape[1]
    H = HEAD
    R = HEADS // KV_HEADS
    L = n * T
    share, win = window(normed_input.shape[2], n)
    vm = pl.BlockSpec(memory_space=pltpu.VMEM)
    dma = pltpu.SemaphoreType.DMA
    out = pl.pallas_call(
        functools.partial(kernel, n, nb),
        out_shape=(
            jax.ShapeDtypeStruct((T, HEADS * H), BF16),
            jax.ShapeDtypeStruct((T, KV_HEADS * H), BF16),
            jax.ShapeDtypeStruct((share, KV_HEADS * H), F32),
        ),
        in_specs=[vm] * 6 + [pl.BlockSpec(memory_space=pltpu.SMEM), vm],
        out_specs=(vm, vm, vm),
        scratch_shapes=[
            pltpu.VMEM((n, T, R * H), BF16),
            pltpu.VMEM((n, T, R * H), BF16),
            pltpu.VMEM((n, T, H), BF16),
            pltpu.VMEM((n, T, H), BF16),
            pltpu.VMEM((n, T, win), BF16),
            pltpu.VMEM((n, 8, T), F32),
            pltpu.VMEM((n, 8, T), F32),
            pltpu.VMEM((H, L), BF16),
            pltpu.VMEM((win, L), BF16),
            pltpu.VMEM((L, H), F32),
            pltpu.VMEM((L, H), F32),
            pltpu.VMEM((n, T, R * H), BF16),
            pltpu.VMEM((n, T, H), BF16),
            pltpu.VMEM((n, L, H), BF16),
            pltpu.VMEM((win, H), F32),
            pltpu.VMEM((n, share, H), BF16),
            pltpu.VMEM((n, share, H), BF16),
            pltpu.VMEM((n, share, H), BF16),
            pltpu.VMEM((n, share, H), BF16),
            pltpu.VMEM((n, T, R * H), BF16),
            pltpu.VMEM((n, T, H), BF16),
            dma((6, n)), dma((6, n)), dma((3, n)), dma((3, n)),
            dma((n,)), dma((n,)), dma((n,)), dma((n,)),
        ],
        compiler_params=pltpu.CompilerParams(
            collective_id=0, has_side_effects=True, vmem_limit_bytes=56 * 1024 * 1024
        ),
    )(
        query_rows[0], key_rows[0], value_rows[0], attn_output[0], output_grad[0], log_norm[0],
        slab_order, normed_input[0],
    )
    return out[0][None], out[1][None], out[2]


def pick(*args):
    n, nb = lax.axis_size("seq"), lax.axis_size("batch")
    fits = n == KV_HEADS and n & (n - 1) == 0 and nb % 2 == 0 and args[0].shape[1] == 128
    return by_heads(n, nb, *args) if fits else local(*args)


def solution(mesh):
    placed = (
        P("batch", "seq", None),
        P("batch", "seq", None),
        P("batch", "seq", None),
        P("batch", "seq", None),
        P("batch", "seq", None),
        P("batch", None, "seq"),
        P("batch", "seq"),
        P("batch", "seq", None),
    )
    return jax.shard_map(
        pick,
        mesh=mesh,
        in_specs=placed,
        out_specs=(P("batch", "seq", None), P("batch", "seq", None), P("seq", None)),
        check_vma=False,
    )
```

```python
import functools
import math

import jax
import jax.numpy as jnp
from jax import lax
from jax.experimental import pallas as pl
from jax.experimental.pallas import tpu as pltpu
from jax.sharding import PartitionSpec as P

HEADS = 16
KV_HEADS = 8
HEAD = 128


SCALE = 144.0 ** (-0.5)


def block_terms(queries, grads, delta, norms, query_pos, key_block, value_block, key_pos):
    keys_count = key_block.shape[0]
    scores = SCALE * jnp.einsum(
        "tgrd,kgd->grtk", queries, key_block, preferred_element_type=jnp.float32
    )
    allowed = key_pos[None, :] <= query_pos[:, None]
    probs = jnp.where(allowed, jnp.exp(scores - norms[..., None]), 0.0)
    dprob = jnp.einsum("tgrd,kgd->grtk", grads, value_block, preferred_element_type=jnp.float32)
    dscore = probs * (dprob - delta[..., None])
    probs_low = probs.astype(jnp.bfloat16)
    dscore_low = dscore.astype(jnp.bfloat16)
    grad_q = SCALE * jnp.einsum(
        "grtk,kgd->tgrd", dscore_low, key_block, preferred_element_type=jnp.float32
    )
    grad_k = SCALE * jnp.einsum(
        "grtk,tgrd->kgd", dscore_low, queries, preferred_element_type=jnp.float32
    )
    grad_v = jnp.einsum("grtk,tgrd->kgd", probs_low, grads, preferred_element_type=jnp.float32)
    return (grad_q, grad_k.reshape(keys_count, -1), grad_v.reshape(keys_count, -1))


def local(
    query_rows, key_rows, value_rows, attn_output, output_grad, log_norm, slab_order, normed_input
):
    tokens = query_rows.shape[1]
    group = HEADS // KV_HEADS
    kv_width = KV_HEADS * HEAD
    slabs = lax.axis_size("seq")
    length = tokens * slabs
    orders = lax.all_gather(slab_order, "seq", axis=1, tiled=True)
    queries = query_rows[0].reshape(tokens, KV_HEADS, group, HEAD)
    grads = output_grad[0].reshape(tokens, KV_HEADS, group, HEAD)
    outputs = attn_output[0].reshape(tokens, KV_HEADS, group, HEAD)
    delta = jnp.transpose(
        jnp.sum(grads.astype(jnp.float32) * outputs.astype(jnp.float32), axis=3), (1, 2, 0)
    )
    norms = log_norm[0].reshape(KV_HEADS, group, tokens)
    offsets = jnp.arange(tokens, dtype=jnp.int32)
    query_pos = slab_order[0, 0] * tokens + offsets
    width = tokens * -(-512 // tokens)
    empty_kv = jnp.zeros((length, kv_width), jnp.float32)
    empty_q = jnp.zeros((tokens, KV_HEADS, group, HEAD), jnp.float32)
    start = jnp.int32(0)
    grad_q = empty_q
    grad_k = empty_kv
    grad_v = empty_kv
    key_part = lax.all_gather(key_rows, "seq", axis=1, tiled=True)
    value_part = lax.all_gather(value_rows, "seq", axis=1, tiled=True)
    count = key_part.shape[1]
    for begin in range(0, count, width):
        finish = min(begin + width, count)
        shards = (finish - begin) // tokens
        first = (start + begin) // tokens
        places = lax.dynamic_slice_in_dim(orders[0], first, shards, 0)
        key_pos = (places[:, None] * tokens + offsets[None, :]).reshape(-1)
        key_block = key_part[0, begin:finish].reshape(-1, KV_HEADS, HEAD)
        value_block = value_part[0, begin:finish].reshape(-1, KV_HEADS, HEAD)
        term_q, term_k, term_v = block_terms(
            queries, grads, delta, norms, query_pos, key_block, value_block, key_pos
        )
        grad_q = grad_q + term_q
        grad_k = lax.dynamic_update_slice_in_dim(grad_k, term_k, begin, 0)
        grad_v = lax.dynamic_update_slice_in_dim(grad_v, term_v, begin, 0)
    grad_q, part_key, part_value = (grad_q, grad_k, grad_v)
    key_sum, value_sum = (
        lax.psum_scatter(
            part_key.astype(jnp.bfloat16), "seq", scatter_dimension=0, tiled=True
        ).astype(jnp.float32),
        lax.psum_scatter(
            part_value.astype(jnp.bfloat16), "seq", scatter_dimension=0, tiled=True
        ).astype(jnp.float32),
    )
    every_grad = lax.all_gather(value_sum.astype(jnp.bfloat16), "seq", axis=0, tiled=True)
    own_columns = lax.all_to_all(normed_input[0], "seq", split_axis=1, concat_axis=0, tiled=True)
    share = own_columns.shape[1]
    slab_parts = jnp.einsum(
        "std,stk->sdk",
        own_columns.reshape(slabs, tokens, share),
        every_grad.reshape(slabs, tokens, kv_width),
        preferred_element_type=jnp.float32,
    )
    rows_total = jnp.sum(slab_parts.astype(jnp.bfloat16).astype(jnp.float32), axis=0)
    weight = lax.psum(rows_total.astype(jnp.bfloat16), "batch").astype(jnp.float32)
    grad_query = grad_q.astype(jnp.bfloat16).reshape(1, tokens, HEADS * HEAD)
    grad_key = key_sum.astype(jnp.bfloat16).reshape(1, tokens, kv_width)
    return (grad_query, grad_key, weight)


MESH = pl.DeviceIdType.MESH
F32 = jnp.float32
BF16 = jnp.bfloat16
NT = (((1,), (1,)), ((), ()))


def xor(a, b, n):
    out = 0
    bit = 1
    while bit < n:
        x, y = lax.rem(lax.div(a, bit), 2), lax.rem(lax.div(b, bit), 2)
        out = out + bit * (x + y - 2 * x * y)
        bit *= 2
    return out


def at(seq, batch):
    return {"seq": seq, "batch": batch}


def window(width, n):
    share = width // n
    step = math.gcd(share, 128)
    return share, -(-(128 - step + share) // 128) * 128


def kernel(
    n, nb, q_ref, k_ref, v_ref, o_ref, g_ref, norm_ref, order_ref, x_ref,
    gq_ref, gk_ref, gw_ref,
    qr, gr, kr, vr, xr, st_src, str_, kt, xt, dk_acc, dv_acc, dq_buf, dk_buf, dv_all,
    prod, up, cr, snd, tot, gq_in, gk_in,
    in_send, in_recv, out_send, out_recv, zu_send, zu_recv, zc_recv, zd_send, fw_send, loc, g_vm, o_vm,
):
    me = lax.axis_index("seq")
    b = lax.axis_index("batch")
    T = k_ref.shape[0]
    H = HEAD
    R = HEADS // KV_HEADS
    share, win = window(x_ref.shape[1], n)
    half = nb // 2
    left = b < half
    is_end = jnp.logical_or(b == 0, b == nb - 1)
    is_mid = jnp.logical_or(b == half - 1, b == half)
    not_end = jnp.logical_not(is_end)
    not_mid = jnp.logical_not(is_mid)
    inner = jnp.where(left, b + 1, b - 1)
    outer = jnp.where(is_end, inner, jnp.where(left, b - 1, b + 1))

    barrier = pltpu.get_barrier_semaphore()
    for t in range(1, n):
        pl.semaphore_signal(barrier, inc=1, device_id=at(xor(me, jnp.int32(t), n), b), device_id_type=MESH)
    pl.semaphore_signal(barrier, inc=1, device_id=at(me, inner), device_id_type=MESH)

    @pl.when(not_end)
    def _():
        pl.semaphore_signal(barrier, inc=1, device_id=at(me, outer), device_id_type=MESH)

    pl.semaphore_wait(barrier, jnp.where(is_end, n, n + 1))

    def cols(who, width):
        return pl.ds(pl.multiple_of(who * width, 128), width)

    def xstart(who):
        return pl.multiple_of(lax.div(who * share, 128) * 128, 128)

    def send_in(kind, t):
        peer = xor(me, jnp.int32(t), n)
        src, dst = {
            0: lambda: (k_ref.at[:, cols(peer, H)], kr.at[me]),
            1: lambda: (v_ref.at[:, cols(peer, H)], vr.at[me]),
            2: lambda: (q_ref.at[:, cols(peer, R * H)], qr.at[me]),
            3: lambda: (g_ref.at[:, cols(peer, R * H)], gr.at[me]),
            4: lambda: (x_ref.at[:, pl.ds(xstart(peer), win)], xr.at[me]),
            5: lambda: (st_src.at[peer], str_.at[me]),
        }[kind]()
        return pltpu.make_async_remote_copy(
            src_ref=src, dst_ref=dst, send_sem=in_send.at[kind, t], recv_sem=in_recv.at[kind, t],
            device_id=at(peer, b), device_id_type=MESH)

    def send_out(kind, t):
        peer = xor(me, jnp.int32(t), n)
        src, dst = {
            0: lambda: (dv_all.at[me], dv_all.at[me]),
            1: lambda: (dk_buf.at[peer], gk_in.at[me]),
            2: lambda: (dq_buf.at[peer], gq_in.at[me]),
        }[kind]()
        return pltpu.make_async_remote_copy(
            src_ref=src, dst_ref=dst, send_sem=out_send.at[kind, t], recv_sem=out_recv.at[kind, t],
            device_id=at(peer, b), device_id_type=MESH)

    for kind in (0, 1):
        for t in range(1, n):
            send_in(kind, t).start()
    for t in range(1, n):
        send_in(2, t).start()
        send_in(3, t).start()

    owns = [
        pltpu.make_async_copy(src, dst, loc.at[j])
        for j, (src, dst) in enumerate((
            (g_ref, g_vm),
            (o_ref, o_vm),
            (k_ref.at[:, cols(me, H)], kr.at[me]),
            (v_ref.at[:, cols(me, H)], vr.at[me]),
            (q_ref.at[:, cols(me, R * H)], qr.at[me]),
            (g_ref.at[:, cols(me, R * H)], gr.at[me]),
            (x_ref.at[:, pl.ds(xstart(me), win)], xr.at[me]),
        ))
    ]
    for own in owns:
        own.start()
    for own in owns[:2]:
        own.wait()

    lane = lax.broadcasted_iota(jnp.int32, (T, 128), 1)
    table = jnp.zeros((T, 128), F32)
    for h in range(HEADS):
        part = g_vm[:, h * H:(h + 1) * H].astype(F32) * o_vm[:, h * H:(h + 1) * H].astype(F32)
        table = jnp.where(lane == h, jnp.sum(part, axis=1, keepdims=True), table)
    delta = jnp.transpose(table)
    base = jnp.full((8 - 2 * R, T), (order_ref[0, 0] * T).astype(F32))
    for h in range(n):
        st_src[h, 0:R, :] = norm_ref[h * R:(h + 1) * R, :]
        st_src[h, R:2 * R, :] = delta[h * R:(h + 1) * R, :]
        st_src[h, 2 * R:8, :] = base
    for t in range(1, n):
        send_in(5, t).start()
    for t in range(1, n):
        send_in(4, t).start()

    for own in owns[2:]:
        own.wait()
    str_[me] = st_src[me]
    dk_acc[...] = jnp.zeros_like(dk_acc)
    dv_acc[...] = jnp.zeros_like(dv_acc)

    for t in range(1, n):
        for kind in (0, 1, 5):
            send_in(kind, t).wait_recv()
    for s in range(n):
        kt[:, s * T:(s + 1) * T] = jnp.transpose(kr[s])

    pair = 2 if n % 2 == 0 else 1
    rows = lax.broadcasted_iota(jnp.int32, (T, R * T), 0).astype(F32)
    qoff = lax.broadcasted_iota(jnp.int32, (1, T), 1).astype(F32)

    def wide(i, first):
        return jnp.concatenate([str_[i, first + r:first + r + 1, :] for r in range(R)], axis=1)

    def per_query(t, carry):
        i = xor(me, t, n)

        @pl.when(t > 0)
        def _():
            send_in(2, t).wait_recv()
            send_in(3, t).wait_recv()

        qb, gb = qr[i], gr[i]
        qs = jnp.concatenate([qb[:, r * H:(r + 1) * H] for r in range(R)], axis=0)
        gs = jnp.concatenate([gb[:, r * H:(r + 1) * H] for r in range(R)], axis=0)
        norms, deltas = wide(i, 0), wide(i, R)
        qpos = str_[i, 2 * R:2 * R + 1, :] + qoff
        qpos = jnp.concatenate([qpos] * R, axis=1)
        dqt = jnp.zeros((H, R * T), F32)
        for s in range(0, n, pair):
            kb = kr[s:s + pair].reshape(pair * T, H)
            vb = vr[s:s + pair].reshape(pair * T, H)
            kpos = jnp.concatenate(
                [rows + jnp.concatenate([str_[s + p, 2 * R:2 * R + 1, :]] * R, axis=1) for p in range(pair)],
                axis=0)
            scores = SCALE * lax.dot_general(kb, qs, NT, preferred_element_type=F32)
            probs = jnp.where(kpos <= qpos, jnp.exp(scores - norms), 0.0)
            dprob = lax.dot_general(vb, gs, NT, preferred_element_type=F32)
            low = (probs * (dprob - deltas)).astype(BF16)
            span = slice(s * T, (s + pair) * T)
            dv_acc[span, :] += jnp.dot(probs.astype(BF16), gs, preferred_element_type=F32)
            dk_acc[span, :] += jnp.dot(low, qs, preferred_element_type=F32)
            dqt = dqt + jnp.dot(kt[:, span], low, preferred_element_type=F32)
        dq = jnp.transpose(dqt * SCALE)
        for r in range(R):
            dq_buf[i, :, r * H:(r + 1) * H] = dq[r * T:(r + 1) * T, :].astype(BF16)
        return carry

    lax.fori_loop(0, n, per_query, 0)

    dv_all[me] = dv_acc[...].astype(BF16)
    for t in range(1, n):
        if t == 1 or t % 2 == 0:
            send_out(0, t).start()
    dk_buf[...] = (dk_acc[...] * SCALE).astype(BF16).reshape(dk_buf.shape)
    for kind in (1, 2):
        for t in range(1, n):
            send_out(kind, t).start()

    def turn(t, carry):
        i = xor(me, t, n)

        @pl.when(t > 0)
        def _():
            send_in(4, t).wait_recv()

        xt[:, pl.ds(pl.multiple_of(i * T, 128), T)] = jnp.transpose(xr[i])
        return carry

    lax.fori_loop(0, n, turn, 0)

    off = pl.multiple_of(me * share - xstart(me), math.gcd(share, 128))

    def cross(c):
        return pltpu.make_async_remote_copy(
            src_ref=snd.at[c], dst_ref=cr.at[c], send_sem=zu_send.at[c], recv_sem=zc_recv.at[c],
            device_id=at(me, inner), device_id_type=MESH)

    def inward(c):
        return pltpu.make_async_remote_copy(
            src_ref=snd.at[c], dst_ref=up.at[c], send_sem=zu_send.at[c], recv_sem=zu_recv.at[c],
            device_id=at(me, inner), device_id_type=MESH)

    def outward(c):
        return pltpu.make_async_remote_copy(
            src_ref=tot.at[c], dst_ref=cr.at[c], send_sem=zd_send.at[c], recv_sem=zc_recv.at[c],
            device_id=at(me, outer), device_id_type=MESH)

    def forward(c):
        head = xor(me, c, n)
        return pltpu.make_async_remote_copy(
            src_ref=dv_all.at[head], dst_ref=dv_all.at[head], send_sem=fw_send.at[c],
            recv_sem=out_recv.at[0, c + 1], device_id=at(xor(me, jnp.int32(1), n), b), device_id_type=MESH)

    def go_up(c):
        @pl.when(c > 0)
        def _():
            send_out(0, c).wait_recv()

        @pl.when(jnp.logical_and(c > 0, lax.rem(c, 2) == 0))
        def _():
            forward(c).start()

        prod[...] = jnp.dot(xt[...], dv_all[xor(me, c, n)], preferred_element_type=F32)

        @pl.when(is_end)
        def _():
            snd[c] = prod[pl.ds(off, share), :].astype(BF16)

        @pl.when(not_end)
        def _():
            inward(c).wait_recv()
            snd[c] = (prod[pl.ds(off, share), :] + up[c].astype(F32)).astype(BF16)

        @pl.when(is_mid)
        def _():
            cross(c).start()

        @pl.when(not_mid)
        def _():
            inward(c).start()

    def go_down(c):
        cross(c).wait_recv()
        head = cols(xor(me, c, n), H)

        @pl.when(is_mid)
        def _():
            tot[c] = (snd[c].astype(F32) + cr[c].astype(F32)).astype(BF16)

        @pl.when(not_mid)
        def _():
            tot[c] = cr[c]

        @pl.when(not_end)
        def _():
            outward(c).start()

        gw_ref[:, head] = tot[c]

    lag = jnp.where(is_mid, 2, n)

    def z_step(c, carry):
        @pl.when(c < n)
        def _():
            go_up(c)

        @pl.when(jnp.logical_and(c >= lag, c < lag + n))
        def _():
            go_down(c - lag)

        return carry

    lax.fori_loop(0, 2 * n, z_step, 0)

    gk_ref[:, cols(me, H)] = dk_buf[me]
    gq_ref[:, cols(me, R * H)] = dq_buf[me]

    def collect(t, carry):
        i = xor(me, t, n)
        send_out(1, t).wait_recv()
        send_out(2, t).wait_recv()
        gk_ref[:, cols(i, H)] = gk_in[i]
        gq_ref[:, cols(i, R * H)] = gq_in[i]
        return carry

    lax.fori_loop(1, n, collect, 0)

    def drain(t, carry):
        for kind in range(6):
            send_in(kind, t).wait_send()
        for kind in (1, 2):
            send_out(kind, t).wait_send()
        even = lax.rem(t, 2) == 0

        @pl.when(jnp.logical_or(t == 1, even))
        def _():
            send_out(0, t).wait_send()

        @pl.when(even)
        def _():
            forward(t).wait_send()

        return carry

    lax.fori_loop(1, n, drain, 0)

    def drain_z(c, carry):
        cross(c).wait_send()

        @pl.when(not_end)
        def _():
            outward(c).wait_send()

        return carry

    lax.fori_loop(0, n, drain_z, 0)


def by_heads(
    n, nb, query_rows, key_rows, value_rows, attn_output, output_grad, log_norm, slab_order, normed_input
):
    T = query_rows.shape[1]
    H = HEAD
    R = HEADS // KV_HEADS
    L = n * T
    share, win = window(normed_input.shape[2], n)
    vm = pl.BlockSpec(memory_space=pltpu.VMEM)
    hbm = pl.BlockSpec(memory_space=pl.ANY)
    dma = pltpu.SemaphoreType.DMA
    out = pl.pallas_call(
        functools.partial(kernel, n, nb),
        out_shape=(
            jax.ShapeDtypeStruct((T, HEADS * H), BF16),
            jax.ShapeDtypeStruct((T, KV_HEADS * H), BF16),
            jax.ShapeDtypeStruct((share, KV_HEADS * H), BF16),
        ),
        in_specs=[hbm] * 5 + [vm, pl.BlockSpec(memory_space=pltpu.SMEM), hbm],
        out_specs=(vm, vm, vm),
        scratch_shapes=[
            pltpu.VMEM((n, T, R * H), BF16),
            pltpu.VMEM((n, T, R * H), BF16),
            pltpu.VMEM((n, T, H), BF16),
            pltpu.VMEM((n, T, H), BF16),
            pltpu.VMEM((n, T, win), BF16),
            pltpu.VMEM((n, 8, T), F32),
            pltpu.VMEM((n, 8, T), F32),
            pltpu.VMEM((H, L), BF16),
            pltpu.VMEM((win, L), BF16),
            pltpu.VMEM((L, H), F32),
            pltpu.VMEM((L, H), F32),
            pltpu.VMEM((n, T, R * H), BF16),
            pltpu.VMEM((n, T, H), BF16),
            pltpu.VMEM((n, L, H), BF16),
            pltpu.VMEM((win, H), F32),
            pltpu.VMEM((n, share, H), BF16),
            pltpu.VMEM((n, share, H), BF16),
            pltpu.VMEM((n, share, H), BF16),
            pltpu.VMEM((n, share, H), BF16),
            pltpu.VMEM((n, T, R * H), BF16),
            pltpu.VMEM((n, T, H), BF16),
            dma((6, n)), dma((6, n)), dma((3, n)), dma((3, n)),
            dma((n,)), dma((n,)), dma((n,)), dma((n,)), dma((n,)), dma((7,)),
            pltpu.VMEM((T, HEADS * H), BF16),
            pltpu.VMEM((T, HEADS * H), BF16),
        ],
        compiler_params=pltpu.CompilerParams(
            collective_id=0, has_side_effects=True, vmem_limit_bytes=56 * 1024 * 1024
        ),
    )(
        query_rows[0], key_rows[0], value_rows[0], attn_output[0], output_grad[0], log_norm[0],
        slab_order, normed_input[0],
    )
    return out[0][None], out[1][None], out[2].astype(F32)


def pick(*args):
    n, nb = lax.axis_size("seq"), lax.axis_size("batch")
    fits = n == KV_HEADS and n & (n - 1) == 0 and nb % 2 == 0 and args[0].shape[1] == 128
    return by_heads(n, nb, *args) if fits else local(*args)


def solution(mesh):
    placed = (
        P("batch", "seq", None),
        P("batch", "seq", None),
        P("batch", "seq", None),
        P("batch", "seq", None),
        P("batch", "seq", None),
        P("batch", None, "seq"),
        P("batch", "seq"),
        P("batch", "seq", None),
    )
    return jax.shard_map(
        pick,
        mesh=mesh,
        in_specs=placed,
        out_specs=(P("batch", "seq", None), P("batch", "seq", None), P("seq", None)),
        check_vma=False,
    )
```
